8 devices in a mesh: dp: 2 (over z, y), sp: 4 (over x, core).
Axes of the slice: x: 2, y: 2, z: 1, core: 2. Of those that a mesh axis runs over, the one named last changes fastest.
Arguments:
- x_in: bfloat16 [8, 4096, 2560], P('dp', 'sp'), parts along dimension 0
- dy_in: bfloat16 [8, 4096, 2560], P('dp', 'sp'), parts along dimension 0
- positions: int32 [8192], P(('dp', 'sp')), parts along dimension 0
- w_q: bfloat16 [2560, 2048], replicated
- w_k: bfloat16 [2560, 1024], replicated
- w_v: bfloat16 [2560, 1024], replicated
- w_o: bfloat16 [2048, 2560], replicated
- w_pre: float32 [2560], replicated
- w_post: float32 [2560], replicated
- q_norm: float32 [256], replicated
- k_norm: float32 [256], replicated
Outputs:
- output 1: bfloat16 [8, 4096, 2560], P('dp', 'sp'), parts along dimension 0
- output 2: bfloat16 [8, 4096, 2560], P('dp', 'sp'), parts along dimension 0
- output 3: bfloat16 [5120, 2048], P('dp'), parts along dimension 0
- output 4: bfloat16 [5120, 1024], P('dp'), parts along dimension 0
- output 5: bfloat16 [5120, 1024], P('dp'), parts along dimension 0
- output 6: bfloat16 [4096, 2560], P('dp'), parts along dimension 0
- output 7: float32 [5120], P('dp'), parts along dimension 0
- output 8: float32 [5120], P('dp'), parts along dimension 0
- output 9: float32 [512], P('dp'), parts along dimension 0
- output 10: float32 [512], P('dp'), parts along dimension 0
There are 2 independent parts. The reference program is written for one: setup_inputs(seed, part) draws one part's arguments, and reference() takes and returns one part's arrays. A program takes and returns all parts, laid end to end along the dimension named above; an argument that names none is the same for every part.
All inputs are finite; a program needn't handle non-finite values.
Results may differ from the reference program's by a relative error of at most 0.02.
Values are sent between devices in bfloat16 or wider.
A program may use at most 1 GiB of HBM per device.

```python
import functools
import jax
import jax.numpy as jnp
from jax import lax

B = 4
SEQ = 4096
D = 2560
H = 8
K = 4
HEAD = 256

EPS = 1e-6
ROPE_BASE = 1000000.0
ROPE_SCALE = 8.0
NEG_BIG = -1e30
Q_ROWS = min(128, SEQ)


def setup_inputs(seed: int = 0, part: int = 0) -> dict:
    base_key = jax.random.key(seed)
    own = jax.random.split(jax.random.fold_in(base_key, part), 4)
    shared = jax.random.split(base_key, 8)
    x_in = jax.random.normal(own[0], (B, SEQ, D), jnp.float32).astype(jnp.bfloat16)
    dy_in = jax.random.normal(own[1], (B, SEQ, D), jnp.float32).astype(jnp.bfloat16)
    start = jax.random.randint(own[2], (1,), 0, 1000)
    gaps = jax.random.randint(own[3], (SEQ,), 1, 5)
    positions = (start + jnp.cumsum(gaps) - gaps[0]).astype(jnp.int32)
    w_q = (jax.random.normal(shared[0], (D, H * HEAD), jnp.float32) * D ** -0.5).astype(jnp.bfloat16)
    w_k = (jax.random.normal(shared[1], (D, K * HEAD), jnp.float32) * D ** -0.5).astype(jnp.bfloat16)
    w_v = (jax.random.normal(shared[2], (D, K * HEAD), jnp.float32) * D ** -0.5).astype(jnp.bfloat16)
    w_o = (jax.random.normal(shared[3], (H * HEAD, D), jnp.float32) * (H * HEAD) ** -0.5).astype(jnp.bfloat16)
    w_pre = 0.3 * jax.random.normal(shared[4], (D,), jnp.float32)
    w_post = 0.3 * jax.random.normal(shared[5], (D,), jnp.float32)
    q_norm = 0.3 + 0.3 * jax.random.normal(shared[6], (HEAD,), jnp.float32)
    k_norm = 0.3 + 0.3 * jax.random.normal(shared[7], (HEAD,), jnp.float32)
    return {'x_in': x_in, 'dy_in': dy_in, 'positions': positions, 'w_q': w_q, 'w_k': w_k, 'w_v': w_v, 'w_o': w_o, 'w_pre': w_pre, 'w_post': w_post, 'q_norm': q_norm, 'k_norm': k_norm}


def rms_scale(x_f32, weight):
    inv_rms = lax.rsqrt(jnp.mean(x_f32 * x_f32, axis=-1, keepdims=True) + EPS)
    return x_f32 * inv_rms * (1.0 + weight)


def norm_rope(heads_f32, weight, cosines, sines):
    half_dim = HEAD // 2
    normed = rms_scale(heads_f32, weight)
    first = normed[..., :half_dim]
    second = normed[..., half_dim:]
    cos_b = cosines[None, :, None, :]
    sin_b = sines[None, :, None, :]
    return jnp.concatenate([first * cos_b - second * sin_b, second * cos_b + first * sin_b], axis=-1)


def attention(q_rot, k_rot, v_heads):
    group = H // K
    blocks = SEQ // Q_ROWS
    q_blocks = jnp.moveaxis(q_rot.reshape(B, blocks, Q_ROWS, K, group, HEAD), 1, 0)
    key_f32 = k_rot.astype(jnp.float32)
    val_f32 = v_heads.astype(jnp.float32)
    col_ids = jnp.arange(SEQ)

    def one_block(item):
        q_blk, index = item
        scores = jnp.einsum('bqkgh,bskh->bkgqs', q_blk.astype(jnp.float32), key_f32) * HEAD ** -0.5
        row_ids = index * Q_ROWS + jnp.arange(Q_ROWS)
        scores = jnp.where(row_ids[:, None] >= col_ids[None, :], scores, NEG_BIG)
        attn_prob = jax.nn.softmax(scores, axis=-1).astype(jnp.bfloat16).astype(jnp.float32)
        return jnp.einsum('bkgqs,bskh->bqkgh', attn_prob, val_f32).astype(jnp.bfloat16)

    block_out = lax.map(jax.checkpoint(one_block), (q_blocks, jnp.arange(blocks)))
    return jnp.moveaxis(block_out, 0, 1).reshape(B, SEQ, H, HEAD)


def forward(positions, x_in, w_q, w_k, w_v, w_o, w_pre, w_post, q_norm, k_norm):
    x_f32 = x_in.astype(jnp.float32)
    normed = rms_scale(x_f32, w_pre).astype(jnp.bfloat16).astype(jnp.float32)
    q_proj = jnp.einsum('bsd,dn->bsn', normed, w_q.astype(jnp.float32)).astype(jnp.bfloat16)
    k_proj = jnp.einsum('bsd,dn->bsn', normed, w_k.astype(jnp.float32)).astype(jnp.bfloat16)
    v_proj = jnp.einsum('bsd,dn->bsn', normed, w_v.astype(jnp.float32)).astype(jnp.bfloat16)
    half_dim = HEAD // 2
    inv_freq = ROPE_BASE ** (-jnp.arange(half_dim, dtype=jnp.float32) * 2.0 / HEAD)
    angles = (positions.astype(jnp.float32) / ROPE_SCALE)[:, None] * inv_freq[None, :]
    cosines = jnp.cos(angles)
    sines = jnp.sin(angles)
    q_rot = norm_rope(q_proj.reshape(B, SEQ, H, HEAD).astype(jnp.float32), q_norm, cosines, sines).astype(jnp.bfloat16)
    k_rot = norm_rope(k_proj.reshape(B, SEQ, K, HEAD).astype(jnp.float32), k_norm, cosines, sines).astype(jnp.bfloat16)
    v_heads = v_proj.reshape(B, SEQ, K, HEAD)
    attn_out = attention(q_rot, k_rot, v_heads)
    proj = jnp.einsum('bsn,nd->bsd', attn_out.reshape(B, SEQ, H * HEAD).astype(jnp.float32), w_o.astype(jnp.float32)).astype(jnp.bfloat16)
    return (x_f32 + rms_scale(proj.astype(jnp.float32), w_post)).astype(jnp.bfloat16)


def reference(x_in, dy_in, positions, w_q, w_k, w_v, w_o, w_pre, w_post, q_norm, k_norm):
    y_out, pullback = jax.vjp(functools.partial(forward, positions), x_in, w_q, w_k, w_v, w_o, w_pre, w_post, q_norm, k_norm)
    grads = pullback(dy_in)
    return (y_out, grads[0], grads[1], grads[2], grads[3], grads[4], grads[5], grads[6], grads[7], grads[8])
```

```python
import functools
import math
import jax
import jax.numpy as jnp
from jax import lax
from jax.experimental import pallas as pl
from jax.experimental.pallas import tpu as pltpu
from jax.sharding import PartitionSpec as P

EPS = 1e-6
ROPE_BASE = 1000000.0
ROPE_SCALE = 8.0
NEG_BIG = -1e30
LOG2E = math.log2(math.e)
BLOCK = 512
NORM_BLOCK = 256
VMEM_LIMIT = 60 * 1024 * 1024

NT = (((1,), (1,)), ((), ()))
NN = (((1,), (0,)), ((), ()))


def dot(lhs, rhs, dims=NN):
    return lax.dot_general(lhs, rhs, dims, preferred_element_type=jnp.float32)


def row_call(body, toks, rows_in, vecs, rows_out, acc_width, flops):
    rows = lambda arr: pl.BlockSpec((NORM_BLOCK, arr.shape[1]), lambda i: (i, 0))
    vec = lambda arr: pl.BlockSpec((1, arr.shape[1]), lambda i: (0, 0))
    out_specs = [rows(arr) for arr in rows_out]
    out_shape = list(rows_out)
    if acc_width:
        out_specs.append(pl.BlockSpec((8, acc_width), lambda i: (0, 0)))
        out_shape.append(jax.ShapeDtypeStruct((8, acc_width), jnp.float32))
    moved = sum(arr.size * arr.dtype.itemsize for arr in list(rows_in) + list(rows_out))
    return pl.pallas_call(
        body,
        grid=(toks // NORM_BLOCK,),
        in_specs=[rows(arr) for arr in rows_in] + [vec(arr) for arr in vecs],
        out_specs=out_specs,
        out_shape=out_shape,
        compiler_params=pltpu.CompilerParams(dimension_semantics=('arbitrary',), vmem_limit_bytes=VMEM_LIMIT),
        cost_estimate=pl.CostEstimate(flops=flops, bytes_accessed=moved, transcendentals=0),
    )(*rows_in, *vecs)


def pre_norm_kernel(x_ref, w_ref, a_ref):
    x = x_ref[...].astype(jnp.float32)
    inv = lax.rsqrt(jnp.mean(x * x, axis=-1, keepdims=True) + EPS)
    a_ref[...] = (x * inv * (1.0 + w_ref[...])).astype(jnp.bfloat16)


def fold_rows(arr):
    return jnp.sum(arr.reshape(-1, 8, arr.shape[1]), axis=0)


def post_norm_kernel(x_ref, proj_ref, dy_ref, w_ref, y_ref, dproj_ref, dw_ref):
    @pl.when(pl.program_id(0) == 0)
    def _():
        dw_ref[...] = jnp.zeros_like(dw_ref)

    gain = 1.0 + w_ref[...]
    proj = proj_ref[...].astype(jnp.float32)
    inv = lax.rsqrt(jnp.mean(proj * proj, axis=-1, keepdims=True) + EPS)
    hat = proj * inv
    y_ref[...] = (x_ref[...].astype(jnp.float32) + hat * gain).astype(jnp.bfloat16)
    dy = dy_ref[...].astype(jnp.float32)
    dw_ref[...] += fold_rows(dy * hat)
    grad = dy * gain
    mean = jnp.mean(grad * hat, axis=-1, keepdims=True)
    dproj_ref[...] = ((grad - hat * mean) * inv).astype(jnp.bfloat16)


def pre_norm_bwd_kernel(x_ref, dn_ref, dy_ref, w_ref, dx_ref, dw_ref):
    @pl.when(pl.program_id(0) == 0)
    def _():
        dw_ref[...] = jnp.zeros_like(dw_ref)

    x = x_ref[...].astype(jnp.float32)
    inv = lax.rsqrt(jnp.mean(x * x, axis=-1, keepdims=True) + EPS)
    hat = x * inv
    grad = dn_ref[...].astype(jnp.float32)
    dw_ref[...] += fold_rows(grad * hat)
    grad = grad * (1.0 + w_ref[...])
    mean = jnp.mean(grad * hat, axis=-1, keepdims=True)
    dx_ref[...] = (dy_ref[...].astype(jnp.float32) + (grad - hat * mean) * inv).astype(jnp.bfloat16)


def like(arr):
    return jax.ShapeDtypeStruct(arr.shape, jnp.bfloat16)


def rope_tables(positions, head):
    half_dim = head // 2
    inv_freq = ROPE_BASE ** (-jnp.arange(half_dim, dtype=jnp.float32) * 2.0 / head)
    angles = (positions.astype(jnp.float32) / ROPE_SCALE)[:, None] * inv_freq[None, :]
    return jnp.cos(angles), jnp.sin(angles)


def norm_rope_kernel(q_ref, k_ref, cos_ref, sin_ref, qn_ref, kn_ref, qo_ref, ko_ref, *, head):
    half = head // 2
    cos = cos_ref[...]
    sin = sin_ref[...]
    for src, weight, dst in ((q_ref, qn_ref, qo_ref), (k_ref, kn_ref, ko_ref)):
        gain = 1.0 + weight[...]
        for h in range(src.shape[1] // head):
            x = src[:, h * head:(h + 1) * head].astype(jnp.float32)
            inv = lax.rsqrt(jnp.mean(x * x, axis=-1, keepdims=True) + EPS)
            n = x * inv * gain
            a, b = n[:, :half], n[:, half:]
            dst[:, h * head:h * head + half] = (a * cos - b * sin).astype(jnp.bfloat16)
            dst[:, h * head + half:(h + 1) * head] = (b * cos + a * sin).astype(jnp.bfloat16)


def norm_rope(q, k, cos, sin, q_norm, k_norm, head):
    toks = q.shape[0]
    rows = lambda width: pl.BlockSpec((NORM_BLOCK, width), lambda i: (i, 0))
    whole = pl.BlockSpec((1, head), lambda i: (0, 0))
    return pl.pallas_call(
        functools.partial(norm_rope_kernel, head=head),
        grid=(toks // NORM_BLOCK,),
        in_specs=[rows(q.shape[1]), rows(k.shape[1]), rows(head // 2), rows(head // 2), whole, whole],
        out_specs=[rows(q.shape[1]), rows(k.shape[1])],
        out_shape=[jax.ShapeDtypeStruct(q.shape, jnp.bfloat16), jax.ShapeDtypeStruct(k.shape, jnp.bfloat16)],
        compiler_params=pltpu.CompilerParams(dimension_semantics=('arbitrary',), vmem_limit_bytes=VMEM_LIMIT),
        cost_estimate=pl.CostEstimate(flops=(q.size + k.size) * 200, bytes_accessed=(q.size + k.size) * 4, transcendentals=0),
        name='norm_rope',
    )(q, k, cos, sin, q_norm.reshape(1, head), k_norm.reshape(1, head))


def norm_rope_bwd_kernel(dq_ref, dk_ref, q_ref, k_ref, cos_ref, sin_ref, qn_ref, kn_ref, dqo_ref, dko_ref, dqn_ref, dkn_ref, *, head):
    half = head // 2
    cos = cos_ref[...]
    sin = sin_ref[...]

    @pl.when(pl.program_id(0) == 0)
    def _():
        dqn_ref[...] = jnp.zeros_like(dqn_ref)
        dkn_ref[...] = jnp.zeros_like(dkn_ref)

    for grad, src, weight, dst, dwn in ((dq_ref, q_ref, qn_ref, dqo_ref, dqn_ref), (dk_ref, k_ref, kn_ref, dko_ref, dkn_ref)):
        gain = 1.0 + weight[...]
        dw_a = jnp.zeros((8, half), jnp.float32)
        dw_b = jnp.zeros((8, half), jnp.float32)
        for h in range(src.shape[1] // head):
            lo = slice(h * head, h * head + half)
            hi = slice(h * head + half, (h + 1) * head)
            xa = src[:, lo].astype(jnp.float32)
            xb = src[:, hi].astype(jnp.float32)
            ga = grad[:, lo].astype(jnp.float32)
            gb = grad[:, hi].astype(jnp.float32)
            inv = lax.rsqrt(jnp.sum(xa * xa + xb * xb, axis=-1, keepdims=True) / head + EPS)
            na = ga * cos + gb * sin
            nb = gb * cos - ga * sin
            xa = xa * inv
            xb = xb * inv
            dw_a = dw_a + jnp.sum((na * xa).reshape(-1, 8, half), axis=0)
            dw_b = dw_b + jnp.sum((nb * xb).reshape(-1, 8, half), axis=0)
            na = na * gain[:, :half]
            nb = nb * gain[:, half:]
            mean = jnp.sum(na * xa + nb * xb, axis=-1, keepdims=True) / head
            dst[:, lo] = ((na - xa * mean) * inv).astype(jnp.bfloat16)
            dst[:, hi] = ((nb - xb * mean) * inv).astype(jnp.bfloat16)
        dwn[:, :half] += dw_a
        dwn[:, half:] += dw_b


def norm_rope_bwd(dq, dk, q, k, cos, sin, q_norm, k_norm, head):
    toks = q.shape[0]
    rows = lambda width: pl.BlockSpec((NORM_BLOCK, width), lambda i: (i, 0))
    whole = pl.BlockSpec((1, head), lambda i: (0, 0))
    acc = pl.BlockSpec((8, head), lambda i: (0, 0))
    dq_o, dk_o, dqn, dkn = pl.pallas_call(
        functools.partial(norm_rope_bwd_kernel, head=head),
        grid=(toks // NORM_BLOCK,),
        in_specs=[rows(q.shape[1]), rows(k.shape[1]), rows(q.shape[1]), rows(k.shape[1]), rows(head // 2), rows(head // 2), whole, whole],
        out_specs=[rows(q.shape[1]), rows(k.shape[1]), acc, acc],
        out_shape=[jax.ShapeDtypeStruct(q.shape, jnp.bfloat16), jax.ShapeDtypeStruct(k.shape, jnp.bfloat16),
                   jax.ShapeDtypeStruct((8, head), jnp.float32), jax.ShapeDtypeStruct((8, head), jnp.float32)],
        compiler_params=pltpu.CompilerParams(dimension_semantics=('arbitrary',), vmem_limit_bytes=VMEM_LIMIT),
        cost_estimate=pl.CostEstimate(flops=(q.size + k.size) * 300, bytes_accessed=(q.size + k.size) * 6, transcendentals=0),
        name='norm_rope_bwd',
    )(dq, dk, q, k, cos, sin, q_norm.reshape(1, head), k_norm.reshape(1, head))
    return dq_o, dk_o, jnp.sum(dqn, axis=0), jnp.sum(dkn, axis=0)


def causal_tile(scores):
    keys = lax.broadcasted_iota(jnp.int32, scores.shape, 0)
    queries = lax.broadcasted_iota(jnp.int32, scores.shape, 1)
    return jnp.where(queries >= keys, scores, NEG_BIG)


def attn_fwd_kernel(q_ref, k_ref, v_ref, o_ref, lse_ref, vt_ref, acc_ref, *, head, per_kv):
    i = pl.program_id(1)
    blk = BLOCK
    c = LOG2E * head ** -0.5

    @pl.when(i == 0)
    def _():
        for t in range(v_ref.shape[0] // blk):
            vt_ref[:, t * blk:(t + 1) * blk] = v_ref[t * blk:(t + 1) * blk, :].astype(jnp.float32).T.astype(jnp.bfloat16)

    qs = [q_ref[:, g * head:(g + 1) * head] for g in range(per_kv)]

    def tile(j, carry, masked, first):
        start = pl.multiple_of(j * blk, blk)
        k_blk = k_ref[pl.ds(start, blk), :]
        vt_blk = vt_ref[:, pl.ds(start, blk)]
        out = []
        scores = [dot(k_blk, qs[g], NT) for g in range(per_kv)]
        if masked:
            scores = [causal_tile(s) for s in scores]
        for g in range(per_kv):
            s = scores[g]
            top = jnp.max(s, axis=0, keepdims=True)
            if not first:
                m_old, l_old = carry[g]
                top = jnp.maximum(top, m_old)
            p = jnp.exp2(s * c - top * c)
            total = jnp.sum(p, axis=0, keepdims=True)
            pv = dot(vt_blk, p.astype(jnp.bfloat16))
            if first:
                acc_ref[g] = pv
            else:
                alpha = jnp.exp2((m_old - top) * c)
                total = total + l_old * alpha
                acc_ref[g] = acc_ref[g] * alpha + pv
            out.append((top, total))
        return tuple(out)

    state = tile(i, None, True, True)
    state = lax.fori_loop(0, i, lambda j, st: tile(j, st, False, False), state)
    for g in range(per_kv):
        top, total = state[g]
        o_ref[:, g * head:(g + 1) * head] = (acc_ref[g] * (1.0 / total)).T.astype(jnp.bfloat16)
        lse_ref[0, g:g + 1, :] = top * c + jnp.log2(total)


def attn_fwd(q, k, v, head):
    toks = q.shape[0]
    kv_heads = k.shape[1] // head
    per_kv = q.shape[1] // k.shape[1]
    wide = per_kv * head
    blocks = toks // BLOCK
    flops = 2 * 2 * toks * toks // 2 * q.shape[1]
    return pl.pallas_call(
        functools.partial(attn_fwd_kernel, head=head, per_kv=per_kv),
        grid=(kv_heads, blocks),
        in_specs=[pl.BlockSpec((BLOCK, wide), lambda h, i: (i, h)),
                  pl.BlockSpec((toks, head), lambda h, i: (0, h)),
                  pl.BlockSpec((toks, head), lambda h, i: (0, h))],
        out_specs=[pl.BlockSpec((BLOCK, wide), lambda h, i: (i, h)),
                   pl.BlockSpec((1, per_kv, BLOCK), lambda h, i: (h, 0, i))],
        out_shape=[jax.ShapeDtypeStruct(q.shape, jnp.bfloat16),
                   jax.ShapeDtypeStruct((kv_heads, per_kv, toks), jnp.float32)],
        scratch_shapes=[pltpu.VMEM((head, toks), jnp.bfloat16), pltpu.VMEM((per_kv, head, BLOCK), jnp.float32)],
        compiler_params=pltpu.CompilerParams(dimension_semantics=('arbitrary', 'arbitrary'), vmem_limit_bytes=VMEM_LIMIT),
        cost_estimate=pl.CostEstimate(flops=2 * flops, bytes_accessed=(q.size + k.size) * 4, transcendentals=0),
        name='attn_fwd',
    )(q, k, v)


def delta_kernel(o_ref, do_ref, delta_ref, *, head, per_kv):
    half = head // 2
    for g in range(per_kv):
        prod = o_ref[:, g * head:(g + 1) * head].astype(jnp.float32) * do_ref[:, g * head:(g + 1) * head].astype(jnp.float32)
        delta_ref[0, g:g + 1, :] = jnp.sum((prod[:, :half] + prod[:, half:]).T, axis=0, keepdims=True)


def attn_delta(o, d_out, kv_heads, head):
    toks, width = o.shape
    wide = width // kv_heads
    rows = min(toks, 1024)
    spec = pl.BlockSpec((rows, wide), lambda h, i: (i, h))
    return pl.pallas_call(
        functools.partial(delta_kernel, head=head, per_kv=wide // head),
        grid=(kv_heads, toks // rows),
        in_specs=[spec, spec],
        out_specs=pl.BlockSpec((1, wide // head, rows), lambda h, i: (h, 0, i)),
        out_shape=jax.ShapeDtypeStruct((kv_heads, wide // head, toks), jnp.float32),
        compiler_params=pltpu.CompilerParams(dimension_semantics=('arbitrary', 'arbitrary'), vmem_limit_bytes=VMEM_LIMIT),
        cost_estimate=pl.CostEstimate(flops=o.size * 200, bytes_accessed=o.size * 4, transcendentals=0),
        name='attn_delta',
    )(o, d_out)


def attn_bwd_kernel(q_ref, do_ref, lse_ref, delta_ref, k_ref, v_ref, dq_ref, dk_ref, dv_ref, dqt_ref, dk_acc, dv_acc, *, head, per_kv, blocks):
    j = pl.program_id(1)
    blk = BLOCK
    scale = head ** -0.5
    c = LOG2E * scale

    @pl.when(j == 0)
    def _():
        dqt_ref[...] = jnp.zeros_like(dqt_ref)

    k_blk = k_ref[...]
    v_blk = v_ref[...]
    kt_blk = k_blk.astype(jnp.float32).T.astype(jnp.bfloat16)

    def tile(i, masked):
        start = pl.multiple_of(i * blk, blk)
        rows = pl.ds(start, blk)
        dk_new, dv_new = None, None
        qs = [q_ref[rows, g * head:(g + 1) * head] for g in range(per_kv)]
        dos = [do_ref[rows, g * head:(g + 1) * head] for g in range(per_kv)]
        scores = [dot(k_blk, qs[g], NT) for g in range(per_kv)]
        d_probs = [dot(v_blk, dos[g], NT) for g in range(per_kv)]
        if masked:
            scores = [causal_tile(s) for s in scores]
        for g in range(per_kv):
            p = jnp.exp2(scores[g] * c - lse_ref[0, g:g + 1, rows])
            ds = (p * (d_probs[g] - delta_ref[0, g:g + 1, rows])).astype(jnp.bfloat16)
            dv_g = dot(p.astype(jnp.bfloat16), dos[g])
            dk_g = dot(ds, qs[g])
            dk_new = dk_g if dk_new is None else dk_new + dk_g
            dv_new = dv_g if dv_new is None else dv_new + dv_g
            dqt_ref[g, :, rows] += dot(kt_blk, ds)
        return dk_new, dv_new

    dk_new, dv_new = tile(j, True)
    dk_acc[...] = dk_new
    dv_acc[...] = dv_new
    own = pl.ds(pl.multiple_of(j * blk, blk), blk)
    for g in range(per_kv):
        dq_ref[:, g * head:(g + 1) * head] = (dqt_ref[g, :, own] * scale).T.astype(jnp.bfloat16)

    def body(i, _):
        dk_new, dv_new = tile(i, False)
        dk_acc[...] += dk_new
        dv_acc[...] += dv_new
        return _

    lax.fori_loop(j + 1, blocks, body, 0)
    dk_ref[...] = (dk_acc[...] * scale).astype(jnp.bfloat16)
    dv_ref[...] = dv_acc[...].astype(jnp.bfloat16)


def attn_bwd(q, k, v, lse, delta, d_out, head):
    toks = q.shape[0]
    kv_heads = k.shape[1] // head
    per_kv = q.shape[1] // k.shape[1]
    wide = per_kv * head
    blocks = toks // BLOCK
    flops = 5 * 2 * toks * toks // 2 * q.shape[1]
    whole = pl.BlockSpec((toks, wide), lambda h, j: (0, h))
    stat = pl.BlockSpec((1, per_kv, toks), lambda h, j: (h, 0, 0))
    kv_spec = pl.BlockSpec((BLOCK, head), lambda h, j: (j, h))
    return pl.pallas_call(
        functools.partial(attn_bwd_kernel, head=head, per_kv=per_kv, blocks=blocks),
        grid=(kv_heads, blocks),
        in_specs=[whole, whole, stat, stat, kv_spec, kv_spec],
        out_specs=[pl.BlockSpec((BLOCK, wide), lambda h, j: (j, h)), kv_spec, kv_spec],
        out_shape=[jax.ShapeDtypeStruct(q.shape, jnp.bfloat16), jax.ShapeDtypeStruct(k.shape, jnp.bfloat16),
                   jax.ShapeDtypeStruct(v.shape, jnp.bfloat16)],
        scratch_shapes=[pltpu.VMEM((per_kv, head, toks), jnp.float32), pltpu.VMEM((BLOCK, head), jnp.float32),
                        pltpu.VMEM((BLOCK, head), jnp.float32)],
        compiler_params=pltpu.CompilerParams(dimension_semantics=('arbitrary', 'arbitrary'), vmem_limit_bytes=VMEM_LIMIT),
        cost_estimate=pl.CostEstimate(flops=2 * flops, bytes_accessed=(q.size + k.size) * 6, transcendentals=0),
        name='attn_bwd',
    )(q, d_out, lse, delta, k, v)


def solution(mesh):
    def to_seqs(arr):
        return lax.all_to_all(arr, 'sp', 0, 0, tiled=True).reshape(-1, arr.shape[2])

    def to_tokens(arr, shape):
        return lax.all_to_all(arr.reshape(shape), 'sp', 0, 0, tiled=True)

    def mm(lhs, rhs, dims):
        return lax.dot_general(lhs, rhs, (dims, ((), ())), preferred_element_type=jnp.float32)

    def reduce_grad(partial_sum):
        shard = lax.psum_scatter(partial_sum, 'sp', scatter_dimension=0, tiled=True)
        return lax.all_gather(shard.astype(jnp.bfloat16), 'sp', axis=0, tiled=True)

    def device_step(x_in, dy_in, positions, w_q, w_k, w_v, w_o, w_pre, w_post, q_norm, k_norm):
        width = x_in.shape[2]
        head = q_norm.shape[0]
        kv_heads = w_k.shape[1] // head
        w_pre = w_pre.reshape(1, width)
        w_post = w_post.reshape(1, width)
        x_seq = to_seqs(x_in)
        dy_seq = to_seqs(dy_in)
        pos_all = lax.all_gather(positions, 'sp', axis=0, tiled=True)
        cosines, sines = rope_tables(pos_all, head)
        toks = x_seq.shape[0]
        normed, = row_call(pre_norm_kernel, toks, [x_seq], [w_pre], [like(x_seq)], 0, x_seq.size * 100)
        q_proj = mm(normed, w_q, ((1,), (0,))).astype(jnp.bfloat16)
        k_proj = mm(normed, w_k, ((1,), (0,))).astype(jnp.bfloat16)
        v_proj = mm(normed, w_v, ((1,), (0,))).astype(jnp.bfloat16)
        q_rot, k_rot = norm_rope(q_proj, k_proj, cosines, sines, q_norm, k_norm, head)
        o_flat, lse = attn_fwd(q_rot, k_rot, v_proj, head)
        proj = mm(o_flat, w_o, ((1,), (0,))).astype(jnp.bfloat16)
        y_seq, d_proj, dw_post = row_call(post_norm_kernel, toks, [x_seq, proj, dy_seq], [w_post], [like(x_seq), like(x_seq)], width, x_seq.size * 300)
        y_out = to_tokens(y_seq, x_in.shape)
        dwo_part = mm(o_flat, d_proj, ((0,), (0,)))
        d_oflat = mm(d_proj, w_o, ((1,), (1,))).astype(jnp.bfloat16)
        dw_o = reduce_grad(dwo_part)
        delta = attn_delta(o_flat, d_oflat, kv_heads, head)
        dq_rot, dk_rot, dv_flat = attn_bwd(q_rot, k_rot, v_proj, lse, delta, d_oflat, head)
        dwv_part = mm(normed, dv_flat, ((0,), (0,)))
        dw_v = reduce_grad(dwv_part)
        dq_flat, dk_flat, dq_norm, dk_norm = norm_rope_bwd(dq_rot, dk_rot, q_proj, k_proj, cosines, sines, q_norm, k_norm, head)
        dwq_part = mm(normed, dq_flat, ((0,), (0,)))
        dw_q = reduce_grad(dwq_part)
        dwk_part = mm(normed, dk_flat, ((0,), (0,)))
        dw_k = reduce_grad(dwk_part)
        d_normed = (mm(dq_flat, w_q, ((1,), (1,))) + mm(dk_flat, w_k, ((1,), (1,)))
                    + mm(dv_flat, w_v, ((1,), (1,)))).astype(jnp.bfloat16)
        dx_seq, dw_pre = row_call(pre_norm_bwd_kernel, toks, [x_seq, d_normed, dy_seq], [w_pre], [like(x_seq)], width, x_seq.size * 200)
        dx_out = to_tokens(dx_seq, x_in.shape)
        small = (jnp.sum(dw_pre, axis=0), jnp.sum(dw_post, axis=0), dq_norm, dk_norm)
        dw_pre, dw_post, dq_norm, dk_norm = lax.psum(small, 'sp')
        return (y_out, dx_out, dw_q, dw_k, dw_v, dw_o, dw_pre, dw_post, dq_norm, dk_norm)

    token_spec = P('dp', 'sp', None)
    return jax.shard_map(device_step, mesh=mesh,
                         in_specs=(token_spec, token_spec, P(('dp', 'sp')), P(None, None), P(None, None), P(None, None), P(None, None), P(None), P(None), P(None), P(None)),
                         out_specs=(token_spec, token_spec, P('dp', None), P('dp', None), P('dp', None), P('dp', None), P('dp'), P('dp'), P('dp'), P('dp')),
                         check_vma=False)
```

```python
import functools
import math
import jax
import jax.numpy as jnp
from jax import lax
from jax.experimental import pallas as pl
from jax.experimental.pallas import tpu as pltpu
from jax.sharding import PartitionSpec as P

EPS = 1e-6
ROPE_BASE = 1000000.0
ROPE_SCALE = 8.0
NEG_BIG = -1e30
LOG2E = math.log2(math.e)
BLOCK = 512
NORM_BLOCK = 512
VMEM_LIMIT = 60 * 1024 * 1024

NT = (((1,), (1,)), ((), ()))
NN = (((1,), (0,)), ((), ()))


def dot(lhs, rhs, dims=NN):
    return lax.dot_general(lhs, rhs, dims, preferred_element_type=jnp.float32)


def row_call(body, toks, rows_in, vecs, rows_out, acc_width, flops):
    rows = lambda arr: pl.BlockSpec((NORM_BLOCK, arr.shape[1]), lambda i: (i, 0))
    vec = lambda arr: pl.BlockSpec((1, arr.shape[1]), lambda i: (0, 0))
    out_specs = [rows(arr) for arr in rows_out]
    out_shape = list(rows_out)
    if acc_width:
        out_specs.append(pl.BlockSpec((8, acc_width), lambda i: (0, 0)))
        out_shape.append(jax.ShapeDtypeStruct((8, acc_width), jnp.float32))
    moved = sum(arr.size * arr.dtype.itemsize for arr in list(rows_in) + list(rows_out))
    return pl.pallas_call(
        body,
        grid=(toks // NORM_BLOCK,),
        in_specs=[rows(arr) for arr in rows_in] + [vec(arr) for arr in vecs],
        out_specs=out_specs,
        out_shape=out_shape,
        compiler_params=pltpu.CompilerParams(dimension_semantics=('arbitrary',), vmem_limit_bytes=VMEM_LIMIT),
        cost_estimate=pl.CostEstimate(flops=flops, bytes_accessed=moved, transcendentals=0),
    )(*rows_in, *vecs)


def pre_norm_kernel(x_ref, w_ref, a_ref):
    x = x_ref[...].astype(jnp.float32)
    inv = lax.rsqrt(jnp.mean(x * x, axis=-1, keepdims=True) + EPS)
    a_ref[...] = (x * inv * (1.0 + w_ref[...])).astype(jnp.bfloat16)


def fold_rows(arr):
    return jnp.sum(arr.reshape(-1, 8, arr.shape[1]), axis=0)


def post_norm_kernel(x_ref, proj_ref, dy_ref, w_ref, y_ref, dproj_ref, dw_ref):
    @pl.when(pl.program_id(0) == 0)
    def _():
        dw_ref[...] = jnp.zeros_like(dw_ref)

    gain = 1.0 + w_ref[...]
    proj = proj_ref[...].astype(jnp.float32)
    inv = lax.rsqrt(jnp.mean(proj * proj, axis=-1, keepdims=True) + EPS)
    hat = proj * inv
    y_ref[...] = (x_ref[...].astype(jnp.float32) + hat * gain).astype(jnp.bfloat16)
    dy = dy_ref[...].astype(jnp.float32)
    dw_ref[...] += fold_rows(dy * hat)
    grad = dy * gain
    mean = jnp.mean(grad * hat, axis=-1, keepdims=True)
    dproj_ref[...] = ((grad - hat * mean) * inv).astype(jnp.bfloat16)


def pre_norm_bwd_kernel(x_ref, dn_ref, dy_ref, w_ref, dx_ref, dw_ref):
    @pl.when(pl.program_id(0) == 0)
    def _():
        dw_ref[...] = jnp.zeros_like(dw_ref)

    x = x_ref[...].astype(jnp.float32)
    inv = lax.rsqrt(jnp.mean(x * x, axis=-1, keepdims=True) + EPS)
    hat = x * inv
    grad = dn_ref[...].astype(jnp.float32)
    dw_ref[...] += fold_rows(grad * hat)
    grad = grad * (1.0 + w_ref[...])
    mean = jnp.mean(grad * hat, axis=-1, keepdims=True)
    dx_ref[...] = (dy_ref[...].astype(jnp.float32) + (grad - hat * mean) * inv).astype(jnp.bfloat16)


def like(arr):
    return jax.ShapeDtypeStruct(arr.shape, jnp.bfloat16)


def rope_tables(positions, head):
    half_dim = head // 2
    inv_freq = ROPE_BASE ** (-jnp.arange(half_dim, dtype=jnp.float32) * 2.0 / head)
    angles = (positions.astype(jnp.float32) / ROPE_SCALE)[:, None] * inv_freq[None, :]
    return jnp.cos(angles), jnp.sin(angles)


def norm_rope_kernel(q_ref, k_ref, cos_ref, sin_ref, qn_ref, kn_ref, qo_ref, ko_ref, *, head):
    half = head // 2
    cos = cos_ref[...]
    sin = sin_ref[...]
    for src, weight, dst in ((q_ref, qn_ref, qo_ref), (k_ref, kn_ref, ko_ref)):
        gain = 1.0 + weight[...]
        for h in range(src.shape[1] // head):
            x = src[:, h * head:(h + 1) * head].astype(jnp.float32)
            inv = lax.rsqrt(jnp.mean(x * x, axis=-1, keepdims=True) + EPS)
            n = x * inv * gain
            a, b = n[:, :half], n[:, half:]
            dst[:, h * head:h * head + half] = (a * cos - b * sin).astype(jnp.bfloat16)
            dst[:, h * head + half:(h + 1) * head] = (b * cos + a * sin).astype(jnp.bfloat16)


def norm_rope(q, k, cos, sin, q_norm, k_norm, head):
    toks = q.shape[0]
    rows = lambda width: pl.BlockSpec((NORM_BLOCK, width), lambda i: (i, 0))
    whole = pl.BlockSpec((1, head), lambda i: (0, 0))
    return pl.pallas_call(
        functools.partial(norm_rope_kernel, head=head),
        grid=(toks // NORM_BLOCK,),
        in_specs=[rows(q.shape[1]), rows(k.shape[1]), rows(head // 2), rows(head // 2), whole, whole],
        out_specs=[rows(q.shape[1]), rows(k.shape[1])],
        out_shape=[jax.ShapeDtypeStruct(q.shape, jnp.bfloat16), jax.ShapeDtypeStruct(k.shape, jnp.bfloat16)],
        compiler_params=pltpu.CompilerParams(dimension_semantics=('arbitrary',), vmem_limit_bytes=VMEM_LIMIT),
        cost_estimate=pl.CostEstimate(flops=(q.size + k.size) * 200, bytes_accessed=(q.size + k.size) * 4, transcendentals=0),
        name='norm_rope',
    )(q, k, cos, sin, q_norm.reshape(1, head), k_norm.reshape(1, head))


def norm_rope_bwd_kernel(dq_ref, dk_ref, dv_ref, q_ref, k_ref, cos_ref, sin_ref, qn_ref, kn_ref, out_ref, dqn_ref, dkn_ref, *, head):
    half = head // 2
    cos = cos_ref[...]
    sin = sin_ref[...]

    @pl.when(pl.program_id(0) == 0)
    def _():
        dqn_ref[...] = jnp.zeros_like(dqn_ref)
        dkn_ref[...] = jnp.zeros_like(dkn_ref)

    q_wide = q_ref.shape[1]
    for grad, src, weight, base, dwn in ((dq_ref, q_ref, qn_ref, 0, dqn_ref), (dk_ref, k_ref, kn_ref, q_wide, dkn_ref)):
        gain = 1.0 + weight[...]
        dw_a = jnp.zeros((8, half), jnp.float32)
        dw_b = jnp.zeros((8, half), jnp.float32)
        for h in range(src.shape[1] // head):
            lo = slice(h * head, h * head + half)
            hi = slice(h * head + half, (h + 1) * head)
            xa = src[:, lo].astype(jnp.float32)
            xb = src[:, hi].astype(jnp.float32)
            ga = grad[:, lo].astype(jnp.float32)
            gb = grad[:, hi].astype(jnp.float32)
            inv = lax.rsqrt(jnp.sum(xa * xa + xb * xb, axis=-1, keepdims=True) / head + EPS)
            na = ga * cos + gb * sin
            nb = gb * cos - ga * sin
            xa = xa * inv
            xb = xb * inv
            dw_a = dw_a + jnp.sum((na * xa).reshape(-1, 8, half), axis=0)
            dw_b = dw_b + jnp.sum((nb * xb).reshape(-1, 8, half), axis=0)
            na = na * gain[:, :half]
            nb = nb * gain[:, half:]
            mean = jnp.sum(na * xa + nb * xb, axis=-1, keepdims=True) / head
            out_ref[:, base + lo.start:base + lo.stop] = ((na - xa * mean) * inv).astype(jnp.bfloat16)
            out_ref[:, base + hi.start:base + hi.stop] = ((nb - xb * mean) * inv).astype(jnp.bfloat16)
        dwn[:, :half] += dw_a
        dwn[:, half:] += dw_b
    out_ref[:, q_wide + k_ref.shape[1]:] = dv_ref[...]


def norm_rope_bwd(dq, dk, dv, q, k, cos, sin, q_norm, k_norm, head, part):
    toks = q.shape[0]
    rows = lambda width: pl.BlockSpec((NORM_BLOCK, width), lambda i: (i, 0))
    piece = lambda width: pl.BlockSpec((NORM_BLOCK, width), lambda i: (i, part))
    whole = pl.BlockSpec((1, head), lambda i: (0, 0))
    acc = pl.BlockSpec((8, head), lambda i: (0, 0))
    qw, kw = dq.shape[1], dk.shape[1]
    wide = qw + 2 * kw
    out, dqn, dkn = pl.pallas_call(
        functools.partial(norm_rope_bwd_kernel, head=head),
        grid=(toks // NORM_BLOCK,),
        in_specs=[rows(qw), rows(kw), rows(kw), piece(qw), piece(kw), rows(head // 2), rows(head // 2), whole, whole],
        out_specs=[rows(wide), acc, acc],
        out_shape=[jax.ShapeDtypeStruct((toks, wide), jnp.bfloat16),
                   jax.ShapeDtypeStruct((8, head), jnp.float32), jax.ShapeDtypeStruct((8, head), jnp.float32)],
        compiler_params=pltpu.CompilerParams(dimension_semantics=('arbitrary',), vmem_limit_bytes=VMEM_LIMIT),
        cost_estimate=pl.CostEstimate(flops=(dq.size + dk.size) * 300, bytes_accessed=(dq.size + dk.size) * 6, transcendentals=0),
        name='norm_rope_bwd',
    )(dq, dk, dv, q, k, cos, sin, q_norm.reshape(1, head), k_norm.reshape(1, head))
    return out, jnp.sum(dqn, axis=0), jnp.sum(dkn, axis=0)


def copy_kernel(src_ref, dst_ref):
    dst_ref[...] = src_ref[...]


def own_copy(arr):
    flat = arr.reshape(-1, arr.shape[-1])
    rows = min(512, flat.shape[0])
    spec = pl.BlockSpec((rows, flat.shape[1]), lambda i: (i, 0))
    return pl.pallas_call(
        copy_kernel,
        grid=(flat.shape[0] // rows,),
        in_specs=[spec],
        out_specs=spec,
        out_shape=like(flat),
        compiler_params=pltpu.CompilerParams(dimension_semantics=('arbitrary',), vmem_limit_bytes=VMEM_LIMIT),
        cost_estimate=pl.CostEstimate(flops=flat.size * 100, bytes_accessed=flat.size * 4, transcendentals=0),
    )(flat).reshape(arr.shape)


def causal_tile(scores, offset=0):
    keys = lax.broadcasted_iota(jnp.int32, scores.shape, 0) - offset
    queries = lax.broadcasted_iota(jnp.int32, scores.shape, 1)
    return jnp.where(queries >= keys, scores, NEG_BIG)


def attn_fwd_kernel(q_ref, k_ref, v_ref, o_ref, lse_ref, vt_ref, acc_ref, *, head, per_kv):
    i = pl.program_id(1)
    blk = BLOCK
    c = LOG2E * head ** -0.5

    @pl.when(i == 0)
    def _():
        for t in range(v_ref.shape[0] // blk):
            vt_ref[:, t * blk:(t + 1) * blk] = v_ref[t * blk:(t + 1) * blk, :].astype(jnp.float32).T.astype(jnp.bfloat16)

    qs = [q_ref[:, g * head:(g + 1) * head] for g in range(per_kv)]

    def tile(j, wide, carry, first):
        start = pl.multiple_of(j * blk, blk)
        span = wide * blk
        k_blk = k_ref[pl.ds(start, span), :]
        vt_blk = vt_ref[:, pl.ds(start, span)]
        out = []
        scores = [dot(k_blk, qs[g], NT) for g in range(per_kv)]
        if first:
            scores = [causal_tile(s, span - blk) for s in scores]
        for g in range(per_kv):
            s = scores[g]
            top = jnp.max(s, axis=0, keepdims=True)
            if not first:
                m_old, l_old = carry[g]
                top = jnp.maximum(top, m_old)
            p = jnp.exp2(s * c - top * c)
            total = jnp.sum(p, axis=0, keepdims=True)
            pv = dot(vt_blk, p.astype(jnp.bfloat16))
            if first:
                acc_ref[g] = pv
            else:
                alpha = jnp.exp2((m_old - top) * c)
                total = total + l_old * alpha
                acc_ref[g] = acc_ref[g] * alpha + pv
            out.append((top, total))
        return tuple(out)

    odd = lax.rem(i, 2)
    state = lax.cond(odd == 1, lambda: tile(i - 1, 2, None, True), lambda: tile(i, 1, None, True))
    state = lax.fori_loop(0, i // 2, lambda j, st: tile(2 * j, 2, st, False), state)
    for g in range(per_kv):
        top, total = state[g]
        o_ref[:, g * head:(g + 1) * head] = (acc_ref[g] * (1.0 / total)).T.astype(jnp.bfloat16)
        lse_ref[0, g:g + 1, :] = top * c + jnp.log2(total)


def attn_fwd(q, k, v, head):
    toks = q.shape[0]
    kv_heads = k.shape[1] // head
    per_kv = q.shape[1] // k.shape[1]
    wide = per_kv * head
    blocks = toks // BLOCK
    flops = 2 * 2 * toks * toks // 2 * q.shape[1]
    return pl.pallas_call(
        functools.partial(attn_fwd_kernel, head=head, per_kv=per_kv),
        grid=(kv_heads, blocks),
        in_specs=[pl.BlockSpec((BLOCK, wide), lambda h, i: (i, h)),
                  pl.BlockSpec((toks, head), lambda h, i: (0, h)),
                  pl.BlockSpec((toks, head), lambda h, i: (0, h))],
        out_specs=[pl.BlockSpec((BLOCK, wide), lambda h, i: (i, h)),
                   pl.BlockSpec((1, per_kv, BLOCK), lambda h, i: (h, 0, i))],
        out_shape=[jax.ShapeDtypeStruct(q.shape, jnp.bfloat16),
                   jax.ShapeDtypeStruct((kv_heads, per_kv, toks), jnp.float32)],
        scratch_shapes=[pltpu.VMEM((head, toks), jnp.bfloat16), pltpu.VMEM((per_kv, head, BLOCK), jnp.float32)],
        compiler_params=pltpu.CompilerParams(dimension_semantics=('arbitrary', 'arbitrary'), vmem_limit_bytes=VMEM_LIMIT),
        cost_estimate=pl.CostEstimate(flops=2 * flops, bytes_accessed=(q.size + k.size) * 4, transcendentals=0),
        name='attn_fwd',
    )(q, k, v)


def delta_kernel(o_ref, do_ref, delta_ref, *, head, per_kv):
    half = head // 2
    for g in range(per_kv):
        prod = o_ref[:, g * head:(g + 1) * head].astype(jnp.float32) * do_ref[:, g * head:(g + 1) * head].astype(jnp.float32)
        delta_ref[0, g:g + 1, :] = jnp.sum((prod[:, :half] + prod[:, half:]).T, axis=0, keepdims=True)


def attn_delta(o, d_out, kv_heads, head):
    toks, width = o.shape
    wide = width // kv_heads
    rows = min(toks, 1024)
    spec = pl.BlockSpec((rows, wide), lambda h, i: (i, h))
    return pl.pallas_call(
        functools.partial(delta_kernel, head=head, per_kv=wide // head),
        grid=(kv_heads, toks // rows),
        in_specs=[spec, spec],
        out_specs=pl.BlockSpec((1, wide // head, rows), lambda h, i: (h, 0, i)),
        out_shape=jax.ShapeDtypeStruct((kv_heads, wide // head, toks), jnp.float32),
        compiler_params=pltpu.CompilerParams(dimension_semantics=('arbitrary', 'arbitrary'), vmem_limit_bytes=VMEM_LIMIT),
        cost_estimate=pl.CostEstimate(flops=o.size * 200, bytes_accessed=o.size * 4, transcendentals=0),
        name='attn_delta',
    )(o, d_out)


def attn_bwd_kernel(q_ref, do_ref, lse_ref, delta_ref, k_ref, v_ref, dq_ref, dk_ref, dv_ref, dqt_ref, dk_acc, dv_acc, *, head, per_kv, blocks):
    j = pl.program_id(1)
    blk = BLOCK
    scale = head ** -0.5
    c = LOG2E * scale

    @pl.when(j == 0)
    def _():
        dqt_ref[...] = jnp.zeros_like(dqt_ref)

    k_blk = k_ref[...]
    v_blk = v_ref[...]
    kt_blk = k_blk.astype(jnp.float32).T.astype(jnp.bfloat16)

    def tile(i, masked):
        start = pl.multiple_of(i * blk, blk)
        rows = pl.ds(start, blk)
        dk_new, dv_new = None, None
        qs = [q_ref[rows, g * head:(g + 1) * head] for g in range(per_kv)]
        dos = [do_ref[rows, g * head:(g + 1) * head] for g in range(per_kv)]
        scores = [dot(k_blk, qs[g], NT) for g in range(per_kv)]
        d_probs = [dot(v_blk, dos[g], NT) for g in range(per_kv)]
        if masked:
            scores = [causal_tile(s) for s in scores]
        for g in range(per_kv):
            p = jnp.exp2(scores[g] * c - lse_ref[0, g:g + 1, rows])
            ds = (p * (d_probs[g] - delta_ref[0, g:g + 1, rows])).astype(jnp.bfloat16)
            dv_g = dot(p.astype(jnp.bfloat16), dos[g])
            dk_g = dot(ds, qs[g])
            dk_new = dk_g if dk_new is None else dk_new + dk_g
            dv_new = dv_g if dv_new is None else dv_new + dv_g
            dqt_ref[g, :, rows] += dot(kt_blk, ds)
        return dk_new, dv_new

    dk_new, dv_new = tile(j, True)
    dk_acc[...] = dk_new
    dv_acc[...] = dv_new
    own = pl.ds(pl.multiple_of(j * blk, blk), blk)
    for g in range(per_kv):
        dq_ref[:, g * head:(g + 1) * head] = (dqt_ref[g, :, own] * scale).T.astype(jnp.bfloat16)

    def body(i, _):
        dk_new, dv_new = tile(i, False)
        dk_acc[...] += dk_new
        dv_acc[...] += dv_new
        return _

    lax.fori_loop(j + 1, blocks, body, 0)
    dk_ref[...] = (dk_acc[...] * scale).astype(jnp.bfloat16)
    dv_ref[...] = dv_acc[...].astype(jnp.bfloat16)


def attn_bwd(q, k, v, lse, delta, d_out, head, part, parts):
    toks = q.shape[0]
    heads = k.shape[1] // head // parts
    per_kv = q.shape[1] // k.shape[1]
    wide = per_kv * head
    blocks = toks // BLOCK
    flops = 5 * 2 * toks * toks // 2 * q.shape[1] // parts
    base = part * heads
    whole = pl.BlockSpec((toks, wide), lambda h, j: (0, base + h))
    stat = pl.BlockSpec((1, per_kv, toks), lambda h, j: (base + h, 0, 0))
    kv_spec = pl.BlockSpec((BLOCK, head), lambda h, j: (j, base + h))
    kv_out = pl.BlockSpec((BLOCK, head), lambda h, j: (j, h))
    kv_shape = jax.ShapeDtypeStruct((toks, heads * head), jnp.bfloat16)
    return pl.pallas_call(
        functools.partial(attn_bwd_kernel, head=head, per_kv=per_kv, blocks=blocks),
        grid=(heads, blocks),
        in_specs=[whole, whole, stat, stat, kv_spec, kv_spec],
        out_specs=[pl.BlockSpec((BLOCK, wide), lambda h, j: (j, h)), kv_out, kv_out],
        out_shape=[jax.ShapeDtypeStruct((toks, heads * wide), jnp.bfloat16), kv_shape, kv_shape],
        scratch_shapes=[pltpu.VMEM((per_kv, head, toks), jnp.float32), pltpu.VMEM((BLOCK, head), jnp.float32),
                        pltpu.VMEM((BLOCK, head), jnp.float32)],
        compiler_params=pltpu.CompilerParams(dimension_semantics=('arbitrary', 'arbitrary'), vmem_limit_bytes=VMEM_LIMIT),
        cost_estimate=pl.CostEstimate(flops=2 * flops, bytes_accessed=(q.size + k.size) * 6 // parts, transcendentals=0),
        name='attn_bwd',
    )(q, d_out, lse, delta, k, v)


def solution(mesh):
    def to_seqs(arr):
        return lax.all_to_all(arr, 'sp', 0, 0, tiled=True).reshape(-1, arr.shape[2])

    def to_tokens(arr, shape):
        return lax.all_to_all(arr.reshape(shape), 'sp', 0, 0, tiled=True)

    def mm(lhs, rhs, dims):
        return lax.dot_general(lhs, rhs, (dims, ((), ())), preferred_element_type=jnp.float32)

    def reduce_grad(partial_sum):
        shard = lax.psum_scatter(partial_sum, 'sp', scatter_dimension=0, tiled=True)
        return lax.all_gather(shard.astype(jnp.bfloat16), 'sp', axis=0, tiled=True)

    def device_step(x_in, dy_in, positions, w_q, w_k, w_v, w_o, w_pre, w_post, q_norm, k_norm):
        width = x_in.shape[2]
        head = q_norm.shape[0]
        kv_heads = w_k.shape[1] // head
        w_pre = w_pre.reshape(1, width)
        w_post = w_post.reshape(1, width)
        pos_all = lax.all_gather(positions, 'sp', axis=0, tiled=True)
        x_in, dy_in, pos_all = lax.optimization_barrier((x_in, dy_in, pos_all))
        x_seq = to_seqs(x_in)
        dy_seq = to_seqs(dy_in)
        cosines, sines = rope_tables(pos_all, head)
        toks = x_seq.shape[0]
        parts = 2
        q_cut, k_cut = w_q.shape[1] // parts, w_k.shape[1] // parts
        w_parts = [jnp.concatenate([w_q[:, part * q_cut:(part + 1) * q_cut], w_k[:, part * k_cut:(part + 1) * k_cut],
                                    w_v[:, part * k_cut:(part + 1) * k_cut]], axis=1) for part in range(parts)]
        x_seq, cosines, sines, *w_parts = lax.optimization_barrier((x_seq, cosines, sines, *w_parts))
        normed, = row_call(pre_norm_kernel, toks, [x_seq], [w_pre], [like(x_seq)], 0, x_seq.size * 100)
        q_proj = mm(normed, w_q, ((1,), (0,))).astype(jnp.bfloat16)
        k_proj = mm(normed, w_k, ((1,), (0,))).astype(jnp.bfloat16)
        v_proj = mm(normed, w_v, ((1,), (0,))).astype(jnp.bfloat16)
        q_rot, k_rot = norm_rope(q_proj, k_proj, cosines, sines, q_norm, k_norm, head)
        o_flat, lse = attn_fwd(q_rot, k_rot, v_proj, head)
        proj = mm(o_flat, w_o, ((1,), (0,))).astype(jnp.bfloat16)
        y_seq, d_proj, dw_post = row_call(post_norm_kernel, toks, [x_seq, proj, dy_seq], [w_post], [like(x_seq), like(x_seq)], width, x_seq.size * 300)
        y_out = to_tokens(y_seq, x_in.shape)
        y_out = own_copy(y_out)
        dwo_part = mm(o_flat, d_proj, ((0,), (0,)))
        d_proj, dwo_part = lax.optimization_barrier((d_proj, dwo_part))
        dw_o = reduce_grad(dwo_part)
        dw_o = own_copy(dw_o)
        d_oflat = mm(d_proj, w_o, ((1,), (1,))).astype(jnp.bfloat16)
        delta = attn_delta(o_flat, d_oflat, kv_heads, head)
        grads, dws, dq_norm, dk_norm = [], [], 0.0, 0.0
        for part in range(parts):
            dq_rot, dk_rot, dv_flat = attn_bwd(q_rot, k_rot, v_proj, lse, delta, d_oflat, head, part, parts)
            grad, dqn, dkn = norm_rope_bwd(dq_rot, dk_rot, dv_flat, q_proj, k_proj, cosines, sines, q_norm, k_norm, head, part)
            dq_norm, dk_norm = dq_norm + dqn, dk_norm + dkn
            grads.append(grad)
            dw_part = mm(normed, grad, ((0,), (0,)))
            if part == 0:
                lse, dw_part = lax.optimization_barrier((lse, dw_part))
            dws.append(reduce_grad(dw_part))
        d_normed = (mm(grads[0], w_parts[0], ((1,), (1,))) + mm(grads[1], w_parts[1], ((1,), (1,)))).astype(jnp.bfloat16)
        dx_seq, dw_pre = row_call(pre_norm_bwd_kernel, toks, [x_seq, d_normed, dy_seq], [w_pre], [like(x_seq)], width, x_seq.size * 200)
        small = (jnp.sum(dw_pre, axis=0), jnp.sum(dw_post, axis=0), dq_norm, dk_norm)
        small = lax.psum(small, 'sp')
        dx_seq, small = lax.optimization_barrier((dx_seq, small))
        dx_out = to_tokens(dx_seq, x_in.shape)
        dw_pre, dw_post, dq_norm, dk_norm = small
        k_end = q_cut + k_cut
        dw_q = jnp.concatenate([dw[:, :q_cut] for dw in dws], axis=1)
        dw_k = jnp.concatenate([dw[:, q_cut:k_end] for dw in dws], axis=1)
        dw_v = jnp.concatenate([dw[:, k_end:] for dw in dws], axis=1)
        return (y_out, dx_out, dw_q, dw_k, dw_v, dw_o, dw_pre, dw_post, dq_norm, dk_norm)

    token_spec = P('dp', 'sp', None)
    return jax.shard_map(device_step, mesh=mesh,
                         in_specs=(token_spec, token_spec, P(('dp', 'sp')), P(None, None), P(None, None), P(None, None), P(None, None), P(None), P(None), P(None), P(None)),
                         out_specs=(token_spec, token_spec, P('dp', None), P('dp', None), P('dp', None), P('dp', None), P('dp'), P('dp'), P('dp'), P('dp')),
                         check_vma=False)
```
